32 devices in a mesh: section: 2 (over core), dp: 16 (over z, y, x).
Axes of the slice: x: 2, y: 2, z: 4, core: 2. Of those that a mesh axis runs over, the one named last changes fastest.
Arguments:
- replay: bfloat16 [2048, 4096], P('dp'), may hold values from -6 to 6
- state_ids: int32 [2048], P('dp'), may hold values from 0 to 2047, as said below
- sampled: int32 [2048, 20], P('dp'), may hold values from 0 to 255
- targets: int32 [2048], P('dp'), may hold values from 0 to 19
- action_table: bfloat16 [256, 4096], replicated, may hold values from -6 to 6
- norm_gain: float32 [2, 4096], P('section'), may hold values from 0.5 to 1.5
- w_up: bfloat16 [2, 4096, 512], P('section', 'dp'), may hold values from -0.09375 to 0.09375
- w_down: bfloat16 [2, 512, 4096], P('section', 'dp'), may hold values from -0.25 to 0.25
Outputs:
- grad_up: float32 [2, 4096, 512], P('section', 'dp')
- grad_down: float32 [2, 512, 4096], P('section', 'dp')
- grad_gain: float32 [2, 4096], P('section')
- loss: float32 [], replicated
The draws below stay inside these ranges and needn't reach their ends.
Inputs may be any that keep to these rules, and one draw needn't show every extreme that they name: state_ids[i] // 128 == i // 128: a state's replay row lies in the same aligned block of 128 rows as the state.
All inputs are finite; a program needn't handle non-finite values.
Results may differ from the reference program's by a relative error of at most 0.011.
Values may be sent and summed in bfloat16 or wider, within the bound.
A program may use at most 128 MiB of HBM per device.

```python
import math
import jax
import jax.numpy as jnp
from jax import lax

D = 4096
FF = 512
VOCAB = 256
SAMPLES = 20
ROWS_DEV = 128
ROWS = 2048
N_LAYERS = 2


def draw_state_ids(key, part):
    offset = jnp.arange(ROWS) // ROWS_DEV * ROWS_DEV
    return (jax.random.randint(key, (ROWS,), 0, ROWS_DEV) + offset).astype(jnp.int32)


def with_ends(entries, key, low, top_value):
    longest = entries.shape.index(max(entries.shape))
    spots = []
    for shift in (0, 1):
        where = [jax.random.randint(jax.random.fold_in(key, axis), (), 0, length) for axis, length in enumerate(entries.shape)]
        where[longest] = (where[longest] + shift) % entries.shape[longest]
        spots.append(tuple(where))
    return entries.at[spots[0]].set(low).at[spots[1]].set(top_value)


def steps_of(rng, shape, cuts, low, high):
    loudness = 1.0
    for dim, blocks in cuts:
        heights = jax.random.uniform(jax.random.fold_in(jax.random.fold_in(rng, 6), dim), (blocks,), jnp.float32, low / len(cuts), high / len(cuts))
        loudness = loudness * jnp.repeat(jnp.exp(heights), shape[dim] // blocks).reshape((-1,) + (1,) * (len(shape) - 1 - dim))
    return loudness


def bell_draw(rng, dims, deviation, limit, shards=(), kind=jnp.bfloat16):
    values = deviation * jax.random.normal(rng, dims, jnp.float32)
    if shards:
        values = values * steps_of(rng, dims, shards, -0.22, 0.18)
    return jnp.clip(values, -limit, limit).astype(kind)


def setup_inputs(seed: int = 0) -> dict:
    arg_keys = jax.random.split(jax.random.key(seed), 9)
    return {
        "replay": bell_draw(arg_keys[0], (ROWS, D), 1.0, 6.0, ((0, 16),)),
        "state_ids": draw_state_ids(jax.random.fold_in(arg_keys[8], 71), 0),
        "sampled": with_ends(jax.random.randint(arg_keys[2], (ROWS, SAMPLES), 0, VOCAB), jax.random.fold_in(arg_keys[2], 1), 0, VOCAB - 1).astype(jnp.int32),
        "targets": with_ends(jax.random.randint(arg_keys[3], (ROWS,), 0, SAMPLES), jax.random.fold_in(arg_keys[3], 1), 0, SAMPLES - 1).astype(jnp.int32),
        "action_table": bell_draw(arg_keys[4], (VOCAB, D), 1.0, 6.0),
        "norm_gain": jnp.clip(1.0 + 0.1 * jax.random.normal(arg_keys[5], (N_LAYERS, D), jnp.float32), 0.5, 1.5),
        "w_up": bell_draw(arg_keys[6], (N_LAYERS, D, FF), D ** -0.5, 0.09375, ((0, 2), (1, 16))),
        "w_down": bell_draw(arg_keys[7], (N_LAYERS, FF, D), FF ** -0.5, 0.25, ((0, 2), (1, 16))),
    }


epsilon = 1e-06
logit_cap = 15.0

def contract_last(left, right):
    return lax.dot_general(left, right, (((1,), (1,)), ((), ())), preferred_element_type=jnp.float32)

def contract_first(left, right):
    return lax.dot_general(left, right, (((0,), (0,)), ((), ())), preferred_element_type=jnp.float32)

def layer_forward(states, gain_row, up_proj, down_proj):
    wide = states.astype(jnp.float32)
    recip = lax.rsqrt(lax.optimization_barrier(jnp.mean(wide * wide, -1, keepdims=True)) + epsilon)
    normed = (wide * recip * gain_row).astype(jnp.bfloat16)
    upper = jnp.dot(normed, up_proj, preferred_element_type=jnp.float32)
    sigm = jax.nn.sigmoid(upper)
    active = (upper * sigm).astype(jnp.bfloat16)
    result = (wide + jnp.dot(active, down_proj, preferred_element_type=jnp.float32)).astype(jnp.bfloat16)
    return (result, (wide, recip, normed, upper, sigm, active))

def layer_backward(grad_out, cache, gain_row, up_proj, down_proj):
    wide, recip, normed, upper, sigm, active = cache
    grad_act = contract_last(grad_out, down_proj)
    grad_upper = (grad_act * sigm * (1.0 + upper * (1.0 - sigm))).astype(jnp.bfloat16)
    grad_norm = contract_last(grad_upper, up_proj)
    scaled = grad_norm * gain_row
    gain_term = lax.optimization_barrier(jnp.sum(grad_norm * wide * recip, 0))
    grad_in = grad_out.astype(jnp.float32) + scaled * recip - wide * recip ** 3 * lax.optimization_barrier(jnp.mean(scaled * wide, -1, keepdims=True))
    return (grad_in.astype(jnp.bfloat16), grad_upper, gain_term)

def head_tail(chosen, targets, scale):
    bent = jnp.tanh(chosen / logit_cap)
    logits = logit_cap * bent
    expo = jnp.exp(logits)
    summed = lax.optimization_barrier(jnp.sum(expo, -1, keepdims=True))
    target_hot = (targets[:, None] == jnp.arange(chosen.shape[1])[None, :]).astype(jnp.float32)
    cross = jnp.log(summed[:, 0]) - lax.optimization_barrier(jnp.sum(logits * target_hot, -1))
    loss_sum = jnp.sum(cross) / ROWS_DEV
    d_logits = (expo / summed - target_hot) / ROWS_DEV
    d_chosen = d_logits * (1.0 - bent * bent) / scale
    return (loss_sum, d_chosen)

def reference(replay, state_ids, sampled, targets, action_table, norm_gain, w_up, w_down):
    picked = jnp.take(replay, state_ids, axis=0)
    embedded = jnp.take(action_table, sampled[:, 0], axis=0)
    hidden = (picked.astype(jnp.float32) + embedded.astype(jnp.float32)).astype(jnp.bfloat16)
    kept_inputs = []
    for layer_idx in range(N_LAYERS):
        kept_inputs.append(hidden)
        hidden, _ = layer_forward(hidden, norm_gain[layer_idx], w_up[layer_idx], w_down[layer_idx])
    scale = math.sqrt(D)
    scores = contract_last(hidden, action_table) / scale
    chosen = jnp.take_along_axis(scores, sampled, axis=1)
    loss_sum, d_chosen = head_tail(chosen, targets, scale)
    row_ids = jnp.arange(scores.shape[0])[:, None]
    d_scores = jnp.zeros(scores.shape, jnp.float32).at[row_ids, sampled].add(d_chosen)
    grad_state = jnp.dot(d_scores.astype(jnp.bfloat16), action_table, preferred_element_type=jnp.float32).astype(jnp.bfloat16)
    ups, downs, gains = ([], [], [])
    for layer_idx in reversed(range(N_LAYERS)):
        _, cache = layer_forward(kept_inputs[layer_idx], norm_gain[layer_idx], w_up[layer_idx], w_down[layer_idx])
        downs.append(contract_first(cache[5], grad_state))
        grad_state_new, grad_upper, gain_term = layer_backward(grad_state, cache, norm_gain[layer_idx], w_up[layer_idx], w_down[layer_idx])
        ups.append(contract_first(cache[2], grad_upper))
        gains.append(gain_term)
        grad_state = grad_state_new
    return (jnp.stack(ups[::-1]), jnp.stack(downs[::-1]), jnp.stack(gains[::-1]), loss_sum)
```

```python
import functools
import math

import jax
import jax.numpy as jnp
from jax import lax
from jax.experimental import pallas as pl
from jax.experimental.pallas import tpu as pltpu
from jax.sharding import PartitionSpec as P

ROWS_DEV = 128
epsilon = 1e-06
logit_cap = 15.0
bf16 = jnp.bfloat16
f32 = jnp.float32


def contract_last(left, right):
    return lax.dot_general(left, right, (((1,), (1,)), ((), ())), preferred_element_type=f32)


def contract_first(left, right):
    return lax.dot_general(left, right, (((0,), (0,)), ((), ())), preferred_element_type=f32)


def dot(left, right):
    return jnp.dot(left, right, preferred_element_type=f32)


def exchange_kernel(size, place, kinds, *refs):
    count = len(kinds)
    ins, outs = refs[:count], refs[count : 2 * count]
    send_sem, recv_sem, own_sem = refs[2 * count :]
    me, target = place()
    barrier = pltpu.get_barrier_semaphore()
    for k in range(1, size):
        pl.semaphore_signal(
            barrier,
            inc=1,
            device_id=target(lax.rem(me + k, size)),
            device_id_type=pl.DeviceIdType.MESH,
        )
    pl.semaphore_wait(barrier, size - 1)
    copies = []
    for a in range(count):
        for k in range(1, size):
            peer = lax.rem(me + k, size)
            copies.append(
                pltpu.make_async_remote_copy(
                    src_ref=ins[a] if kinds[a] else ins[a].at[peer],
                    dst_ref=outs[a].at[me],
                    send_sem=send_sem.at[a, k],
                    recv_sem=recv_sem.at[a, k],
                    device_id=target(peer),
                    device_id_type=pl.DeviceIdType.MESH,
                )
            )
            copies[-1].start()
    own = []
    for a in range(count):
        own.append(
            pltpu.make_async_copy(
                ins[a] if kinds[a] else ins[a].at[me], outs[a].at[me], own_sem.at[a]
            )
        )
        own[-1].start()
    for copy in own:
        copy.wait()
    for copy in copies:
        copy.wait()


class Groups:
    def __init__(self, sections, devices):
        self.sections = sections
        outer = 1
        while outer * outer < devices:
            outer *= 2
        self.outer, self.inner = outer, devices // outer
        self.calls = 0

    def place_outer(self):
        pos = lax.axis_index("dp")
        low = lax.rem(pos, self.inner)
        return lax.div(pos, self.inner), lambda p: {"dp": p * self.inner + low}

    def place_inner(self):
        pos = lax.axis_index("dp")
        low = lax.rem(pos, self.inner)
        return low, lambda p: {"dp": pos - low + p}

    def place_section(self):
        return lax.axis_index("section"), lambda p: {"section": p}

    def run(self, size, place, gathers, swaps):
        arrays = list(gathers) + list(swaps)
        kinds = [True] * len(gathers) + [False] * len(swaps)
        shapes = [
            jax.ShapeDtypeStruct(((size,) + x.shape) if g else x.shape, x.dtype)
            for x, g in zip(arrays, kinds)
        ]
        ident = self.calls
        self.calls += 1
        spec = pl.BlockSpec(memory_space=pltpu.VMEM)
        return pl.pallas_call(
            functools.partial(exchange_kernel, size, place, kinds),
            out_shape=shapes,
            in_specs=[spec] * len(arrays),
            out_specs=[spec] * len(arrays),
            scratch_shapes=[
                pltpu.SemaphoreType.DMA((len(arrays), size)),
                pltpu.SemaphoreType.DMA((len(arrays), size)),
                pltpu.SemaphoreType.DMA((len(arrays),)),
            ],
            compiler_params=pltpu.CompilerParams(collective_id=ident, has_side_effects=True),
        )(*arrays)

    def over_outer(self, gathers=(), swaps=()):
        return self.run(self.outer, self.place_outer, gathers, swaps)

    def over_inner(self, gathers=(), swaps=()):
        return self.run(self.inner, self.place_inner, gathers, swaps)

    def over_section(self, gathers=(), swaps=()):
        return self.run(self.sections, self.place_section, gathers, swaps)


def head_tail(chosen, targets, scale):
    bent = jnp.tanh(chosen / logit_cap)
    logits = logit_cap * bent
    expo = jnp.exp(logits)
    summed = jnp.sum(expo, -1, keepdims=True)
    target_hot = (targets[:, None] == jnp.arange(chosen.shape[1])[None, :]).astype(f32)
    cross = jnp.log(summed[:, 0]) - jnp.sum(logits * target_hot, -1)
    loss_sum = jnp.sum(cross) / ROWS_DEV
    d_logits = (expo / summed - target_hot) / ROWS_DEV
    d_chosen = d_logits * (1.0 - bent * bent) / scale
    return (loss_sum, d_chosen)


def on_device(replay, state_ids, sampled, targets, action_table, norm_gain, w_up, w_down):
    sections = lax.axis_size("section")
    groups = Groups(sections, lax.axis_size("dp"))
    outer, inner = groups.outer, groups.inner
    section_pos = lax.axis_index("section")
    dp_pos = lax.axis_index("dp")
    outer_pos = dp_pos // inner
    held_rows, width = replay.shape
    rows = held_rows // sections
    vocab = action_table.shape[0]
    cut = width // outer
    ff = w_up.shape[2]
    ff_held = w_down.shape[1]
    group_rows = outer * rows
    scale = math.sqrt(width)

    def my_rows(x):
        return lax.dynamic_slice_in_dim(x, section_pos * rows, rows, 0)

    def my_cut(x):
        return lax.dynamic_slice_in_dim(x, outer_pos * cut, cut, 1)

    def to_cuts(x):
        return x.reshape(x.shape[0], outer, cut).transpose(1, 0, 2)

    ids = my_rows(state_ids) - dp_pos * held_rows
    picks = my_rows(sampled)
    marks = my_rows(targets)
    table_cut = my_cut(action_table)
    id_hot = (ids[:, None] == jnp.arange(held_rows)[None, :]).astype(bf16)
    taken_hot = (picks[:, 0:1] == jnp.arange(vocab)[None, :]).astype(bf16)
    start = (dot(id_hot, replay) + dot(taken_hot, action_table)).astype(bf16)
    start_wide = start.astype(f32)
    start_recip = lax.rsqrt(jnp.mean(start_wide * start_wide, -1, keepdims=True) + epsilon)

    state_cuts, down_cuts = groups.over_outer(swaps=(to_cuts(start), to_cuts(w_down[0])))
    up_all, down_all = groups.over_inner(
        gathers=(w_up[0], down_cuts.reshape(outer * ff_held, cut))
    )
    up_cut = up_all.reshape(cut, ff)
    down_cut = (
        down_all.reshape(inner, outer, ff_held, cut).transpose(1, 0, 2, 3).reshape(ff, cut)
    )
    ups, downs, gains = groups.over_section(gathers=(up_cut, down_cut, my_cut(norm_gain)))

    state = state_cuts.reshape(group_rows, cut)
    kept = []
    for layer in range(sections):
        wide = state.astype(f32)
        scaled = wide * gains[layer]
        part = dot(scaled.astype(bf16), ups[layer]).astype(bf16).reshape(outer, rows, ff)
        if layer == 0:
            (parts,) = groups.over_outer(swaps=(part,))
            recip = start_recip
        else:
            squares = jnp.sum(wide * wide, -1).reshape(outer, 1, rows)
            parts, squares = groups.over_outer(swaps=(part, squares))
            recip = lax.rsqrt(jnp.sum(squares, 0).reshape(rows, 1) / width + epsilon)
        upper = jnp.sum(parts.astype(f32), 0) * recip
        active = (upper * jax.nn.sigmoid(upper)).astype(bf16)
        (actives,) = groups.over_outer(gathers=(active,))
        actives = actives.reshape(group_rows, ff)
        kept.append((state, recip, upper, actives))
        state = (wide + dot(actives, downs[layer])).astype(bf16)

    score_part = contract_last(state, table_cut).reshape(outer, rows, vocab)
    (score_parts,) = groups.over_outer(swaps=(score_part,))
    scores = jnp.sum(score_parts, 0) / scale
    hot = picks[:, :, None] == jnp.arange(vocab)[None, None, :]
    chosen = jnp.sum(jnp.where(hot, scores[:, None, :], 0.0), -1)
    loss_sum, d_chosen = head_tail(chosen, marks, scale)
    d_scores = jnp.sum(jnp.where(hot, d_chosen[:, :, None], 0.0), 1).astype(bf16)
    (d_all,) = groups.over_outer(gathers=(d_scores,))
    grad = dot(d_all.reshape(group_rows, vocab), table_cut).astype(bf16)

    grads_up, grads_down, grads_gain = [], [], []
    for layer in reversed(range(sections)):
        state, recip, upper, actives = kept[layer]
        part = contract_last(grad, downs[layer]).astype(bf16).reshape(outer, rows, ff)
        (parts,) = groups.over_outer(swaps=(part,))
        sigm = jax.nn.sigmoid(upper)
        d_upper = (
            jnp.sum(parts.astype(f32), 0) * sigm * (1.0 + upper * (1.0 - sigm))
        ).astype(bf16)
        pull = jnp.sum(d_upper.astype(f32) * upper, -1, keepdims=True) * recip * recip / width
        d_uppers, recips, pulls = groups.over_outer(
            gathers=(d_upper, recip.reshape(1, rows), pull.reshape(1, rows))
        )
        d_uppers = d_uppers.reshape(group_rows, ff)
        recips = recips.reshape(group_rows, 1)
        pulls = pulls.reshape(group_rows, 1)
        wide = state.astype(f32)
        ready = wide * recips
        d_normed = contract_last(d_uppers, ups[layer])
        grads_gain.append(jnp.sum(d_normed * ready, 0))
        normed = (ready * gains[layer]).astype(bf16)
        grads_up.append(contract_first(normed, d_uppers).astype(bf16))
        grads_down.append(contract_first(actives, grad).astype(bf16))
        if layer:
            grad = (
                grad.astype(f32) + d_normed * gains[layer] * recips - wide * pulls
            ).astype(bf16)

    gain_rows = jnp.stack(grads_gain[::-1])[:, None, :]
    loss_rows = jnp.broadcast_to(loss_sum, (sections, 1, 128))
    small = jnp.concatenate([gain_rows, loss_rows], -1)
    up_got, down_got, small_got = groups.over_section(
        swaps=(jnp.stack(grads_up[::-1]), jnp.stack(grads_down[::-1]), small)
    )
    up_mine = jnp.sum(up_got.astype(f32), 0).astype(bf16).reshape(inner, cut // inner, ff)
    down_mine = (
        jnp.sum(down_got.astype(f32), 0)
        .astype(bf16)
        .reshape(outer, inner, ff_held, cut)
        .transpose(1, 0, 2, 3)
        .reshape(inner, outer * ff_held, cut)
    )
    small_got, up_got, down_got = groups.over_inner(
        gathers=(jnp.sum(small_got, 0),), swaps=(up_mine, down_mine)
    )
    grad_up = jnp.sum(up_got.astype(f32), 0)
    down_full = jnp.sum(down_got.astype(f32), 0).astype(bf16).reshape(outer, ff_held, cut)
    small_got, down_got = groups.over_outer(
        gathers=(jnp.sum(small_got, 0),), swaps=(down_full,)
    )
    grad_down = down_got.transpose(1, 0, 2).reshape(ff_held, width).astype(f32)
    grad_gain = small_got[:, 0, :cut].reshape(1, width)
    loss = jnp.sum(small_got[:, 0, cut])
    return (grad_up[None], grad_down[None], grad_gain, loss)


def solution(mesh):
    return jax.shard_map(
        on_device,
        mesh=mesh,
        in_specs=(
            P("dp", None),
            P("dp"),
            P("dp", None),
            P("dp"),
            P(),
            P("section", None),
            P("section", "dp", None),
            P("section", "dp", None),
        ),
        out_specs=(P("section", "dp", None), P("section", "dp", None), P("section", None), P()),
        check_vma=False,
    )
```

```python
import functools
import math

import jax
import jax.numpy as jnp
from jax import lax
from jax.experimental import pallas as pl
from jax.experimental.pallas import tpu as pltpu
from jax.sharding import PartitionSpec as P

ROWS_DEV = 128
epsilon = 1e-06
logit_cap = 15.0
bf16 = jnp.bfloat16
f32 = jnp.float32


def contract_last(left, right):
    return lax.dot_general(left, right, (((1,), (1,)), ((), ())), preferred_element_type=f32)


def contract_first(left, right):
    return lax.dot_general(left, right, (((0,), (0,)), ((), ())), preferred_element_type=f32)


def dot(left, right):
    return jnp.dot(left, right, preferred_element_type=f32)


def spread(rows, column, axis):
    here = lax.broadcasted_iota(jnp.int32, (rows, rows), 0)
    there = lax.broadcasted_iota(jnp.int32, (rows, rows), 1)
    wide = jnp.broadcast_to(column, (rows, rows))
    return jnp.sum(jnp.where(here == there, wide, 0.0), axis, keepdims=True)


class Group:
    def __init__(self, size, me, target):
        self.size, self.me, self.target = size, me, target

    def copy(self, k, source, dest, send_sem, recv_sem):
        peer = lax.rem(self.me + k, self.size)
        made = pltpu.make_async_remote_copy(
            src_ref=source(peer),
            dst_ref=dest,
            send_sem=send_sem,
            recv_sem=recv_sem,
            device_id=self.target(peer),
            device_id_type=pl.DeviceIdType.MESH,
        )
        made.start()
        return made

    def fan(self, source, dest, sems):
        return [
            self.copy(k, source, dest, sems.at[0, k], sems.at[1, k])
            for k in range(1, self.size)
        ]


def groups_of(outer, inner, sections):
    pos = lax.axis_index("dp")
    high, low = lax.div(pos, inner), lax.rem(pos, inner)
    return (
        Group(outer, high, lambda p: {"dp": p * inner + low}),
        Group(inner, low, lambda p: {"dp": pos - low + p}),
        Group(sections, lax.axis_index("section"), lambda p: {"section": p}),
    )


def greet(*groups):
    barrier = pltpu.get_barrier_semaphore()
    for group in groups:
        for k in range(1, group.size):
            pl.semaphore_signal(
                barrier,
                inc=1,
                device_id=group.target(lax.rem(group.me + k, group.size)),
                device_id_type=pl.DeviceIdType.MESH,
            )
    pl.semaphore_wait(barrier, sum(group.size - 1 for group in groups))


def local(source, dest, sem):
    made = pltpu.make_async_copy(source, dest, sem)
    made.start()
    return made


def land(copies):
    for copy in copies:
        copy.wait_recv()


def drain(copies):
    for copy in copies:
        copy.wait_send()


def stage_kernel(dims, start, down, up, gain, state, ups, downs, gains, sems, pass_sems, own_sems):
    across, within, between = groups_of(*dims)
    z, j, s = across.me, within.me, between.me
    greet(across, within, between)
    down_cuts = across.fan(lambda p: down.at[p], downs.at[s, z, j], sems.at[0])
    up_rows = within.fan(lambda p: up, ups.at[s, j], sems.at[1])
    states = across.fan(lambda p: start.at[p], state.at[z], sems.at[2])
    sent = between.fan(lambda p: gain, gains.at[s], sems.at[3])
    sent += between.fan(lambda p: up, ups.at[s, j], pass_sems.at[0, 0])
    down_own = local(down.at[z], downs.at[s, z, j], own_sems.at[0])
    own = [
        local(up, ups.at[s, j], own_sems.at[1]),
        local(start.at[z], state.at[z], own_sems.at[2]),
        local(gain, gains.at[s], own_sems.at[3]),
    ]
    down_own.wait()
    land(down_cuts)
    mine = downs.at[s, :, j]
    down_rows = within.fan(lambda p: mine, mine, sems.at[4])
    sent += between.fan(lambda p: mine, mine, pass_sems.at[1, 0])
    for number, rows in ((0, up_rows), (1, down_rows)):
        for k in range(1, within.size):
            rows[k - 1].wait_recv()
            giver = lax.rem(j + within.size - k, within.size)
            piece = ups.at[s, giver] if number == 0 else downs.at[s, :, giver]
            sent += between.fan(lambda p: piece, piece, pass_sems.at[number, k])
    land(states + sent)
    drain(down_cuts + up_rows + states + down_rows + sent)
    for copy in own:
        copy.wait()


def forward_kernel(dims, width, first, parts, stat, upper, actives, recips, recip, got, stats, row, mine, sems, own_sems):
    across, _, _ = groups_of(*dims)
    z, size = across.me, across.size
    rows = upper.shape[0]
    greet(across)
    sent = across.fan(lambda p: parts.at[p], got.at[z], sems.at[0])
    if not first:
        sent += across.fan(lambda p: stat.at[p], stats.at[z], sems.at[1])
    own = local(parts.at[z], got.at[z], own_sems.at[0])
    own.wait()
    if not first:
        own_stat = local(stat.at[z], stats.at[z], own_sems.at[1])
        own_stat.wait()
    land(sent)
    if first:
        squares = stat[...]
    else:
        squares = spread(rows, jnp.sum(stats[...], 0), 1)
    factor = lax.rsqrt(squares / width + epsilon)
    recip[...] = factor
    total = jnp.sum(got[...].astype(f32), 0) * factor
    active = (total * jax.nn.sigmoid(total)).astype(bf16)
    mine[...] = active
    row[...] = spread(rows, factor, 0)
    upper[...] = total
    more = across.fan(lambda p: mine, actives.at[z], sems.at[2])
    more += across.fan(lambda p: row, recips.at[z], sems.at[3])
    ends = [
        local(mine, actives.at[z], own_sems.at[2]),
        local(row, recips.at[z], own_sems.at[3]),
    ]
    land(more)
    drain(sent + more)
    for copy in ends:
        copy.wait()


def backward_kernel(dims, width, parts, upper, recip, d_uppers, pulls, got, row, mine, sems, own_sems):
    across, _, _ = groups_of(*dims)
    z = across.me
    rows = upper.shape[0]
    greet(across)
    sent = across.fan(lambda p: parts.at[p], got.at[z], sems.at[0])
    own = local(parts.at[z], got.at[z], own_sems.at[0])
    value = upper[...]
    sigm = jax.nn.sigmoid(value)
    slope = sigm * (1.0 + value * (1.0 - sigm))
    own.wait()
    land(sent)
    d_upper = (jnp.sum(got[...].astype(f32), 0) * slope).astype(bf16)
    mine[...] = d_upper
    factor = recip[...]
    pull = jnp.sum(d_upper.astype(f32) * value, -1, keepdims=True) * factor * factor / width
    row[...] = spread(rows, pull, 0)
    more = across.fan(lambda p: mine, d_uppers.at[z], sems.at[1])
    more += across.fan(lambda p: row, pulls.at[z], sems.at[2])
    ends = [
        local(mine, d_uppers.at[z], own_sems.at[1]),
        local(row, pulls.at[z], own_sems.at[2]),
    ]
    land(more)
    drain(sent + more)
    for copy in ends:
        copy.wait()


def head_kernel(dims, scale, parts, picks, marks, grads, loss, got, mine, sems, own_sems):
    across, _, _ = groups_of(*dims)
    z = across.me
    rows, samples = picks.shape
    vocab = parts.shape[2]
    greet(across)
    sent = across.fan(lambda p: parts.at[p], got.at[z], sems.at[0])
    own = local(parts.at[z], got.at[z], own_sems.at[0])
    own.wait()
    land(sent)
    scores = jnp.sum(got[...], 0) / scale
    actions = lax.broadcasted_iota(jnp.int32, (rows, vocab), 1)
    choice = picks[...]
    chosen = jnp.concatenate(
        [
            jnp.sum(jnp.where(choice[:, k : k + 1] == actions, scores, 0.0), -1, keepdims=True)
            for k in range(samples)
        ],
        1,
    )
    bent = jnp.tanh(chosen / logit_cap)
    logits = logit_cap * bent
    expo = jnp.exp(logits)
    summed = jnp.sum(expo, -1, keepdims=True)
    order = lax.broadcasted_iota(jnp.int32, (rows, samples), 1)
    hot = jnp.where(marks[...] == order, 1.0, 0.0)
    cross = jnp.log(summed) - jnp.sum(logits * hot, -1, keepdims=True)
    loss[...] = jnp.broadcast_to(jnp.sum(cross, 0, keepdims=True) / ROWS_DEV, loss.shape)
    d_chosen = (expo / summed - hot) / ROWS_DEV * (1.0 - bent * bent) / scale
    d_scores = jnp.zeros((rows, vocab), f32)
    for k in range(samples):
        d_scores += jnp.where(choice[:, k : k + 1] == actions, d_chosen[:, k : k + 1], 0.0)
    mine[...] = d_scores.astype(bf16)
    more = across.fan(lambda p: mine, grads.at[z], sems.at[1])
    end = local(mine, grads.at[z], own_sems.at[1])
    land(more)
    drain(sent + more)
    end.wait()


def finish_kernel(
    dims, up, down, small, grad_up, down_out, small_out,
    up_got, down_got, small_got, up_sum, down_sum, small_sum,
    up_rows, down_rows, small_rows, down_full, small_full, sems, own_sems,
):
    across, within, between = groups_of(*dims)
    z, j, s = across.me, within.me, between.me
    greet(across, within, between)

    def total(mine, got, group):
        value = mine.astype(f32)
        for k in range(1, group.size):
            value += got[k - 1].astype(f32)
        return value

    def swap(group, source, got, sems):
        return [
            group.copy(k, source, got.at[k - 1], sems.at[0, k], sems.at[1, k])
            for k in range(1, group.size)
        ]

    downs = swap(between, lambda p: down.at[p], down_got, sems.at[0])
    ups = swap(between, lambda p: up.at[p], up_got, sems.at[1])
    smalls = swap(between, lambda p: small.at[p], small_got, sems.at[2])
    land(downs)
    for part in range(across.size):
        value = down[s, part].astype(f32)
        for k in range(1, between.size):
            value += down_got[k - 1, part].astype(f32)
        down_sum[part] = value.astype(bf16)
    down_in = swap(within, lambda p: down_sum.at[:, p], down_rows, sems.at[3])
    land(smalls)
    small_sum[...] = total(small[s], small_got, between)
    small_in = swap(within, lambda p: small_sum, small_rows, sems.at[4])
    land(ups)
    for part in range(within.size):
        value = up[s, part].astype(f32)
        for k in range(1, between.size):
            value += up_got[k - 1, part].astype(f32)
        up_sum[part] = value.astype(bf16)
    up_in = swap(within, lambda p: up_sum.at[p], up_rows, sems.at[5])
    land(down_in)
    down_full[...] = total(down_sum[:, j], down_rows, within).astype(bf16)
    down_ends = across.fan(lambda p: down_full.at[p], down_out.at[z], sems.at[6])
    land(small_in)
    small_full[...] = total(small_sum[...], small_rows, within)
    small_ends = across.fan(lambda p: small_full, small_out.at[z], sems.at[7])
    own = [
        local(down_full.at[z], down_out.at[z], own_sems.at[0]),
        local(small_full, small_out.at[z], own_sems.at[1]),
    ]
    land(up_in)
    grad_up[...] = total(up_sum[j], up_rows, within)
    land(down_ends + small_ends)
    drain(downs + ups + smalls + down_in + small_in + up_in + down_ends + small_ends)
    for copy in own:
        copy.wait()


def call(ident, kernel, args, outs, scratch, sem_shapes):
    spec = pl.BlockSpec(memory_space=pltpu.VMEM)
    return pl.pallas_call(
        kernel,
        out_shape=[jax.ShapeDtypeStruct(shape, kind) for shape, kind in outs],
        in_specs=[spec] * len(args),
        out_specs=[spec] * len(outs),
        scratch_shapes=[pltpu.VMEM(shape, kind) for shape, kind in scratch]
        + [pltpu.SemaphoreType.DMA(shape) for shape in sem_shapes],
        compiler_params=pltpu.CompilerParams(collective_id=ident, has_side_effects=True),
    )(*args)


def on_device(replay, state_ids, sampled, targets, action_table, norm_gain, w_up, w_down):
    sections = lax.axis_size("section")
    devices = lax.axis_size("dp")
    outer = 1
    while outer * outer < devices:
        outer *= 2
    inner = devices // outer
    dims = (outer, inner, sections)
    top = max(dims)
    section_pos = lax.axis_index("section")
    dp_pos = lax.axis_index("dp")
    outer_pos = dp_pos // inner
    held_rows, width = replay.shape
    rows = held_rows // sections
    vocab = action_table.shape[0]
    cut = width // outer
    ff = w_up.shape[2]
    up_held = w_up.shape[1]
    ff_held = w_down.shape[1]
    group_rows = outer * rows
    scale = math.sqrt(width)
    small_width = cut + 128

    def my_rows(x):
        return lax.dynamic_slice_in_dim(x, section_pos * rows, rows, 0)

    def my_cut(x):
        return lax.dynamic_slice_in_dim(x, outer_pos * cut, cut, 1)

    def to_cuts(x):
        return x.reshape(x.shape[0], outer, cut).transpose(1, 0, 2)

    ids = my_rows(state_ids) - dp_pos * held_rows
    picks = my_rows(sampled)
    marks = my_rows(targets)
    table_cut = my_cut(action_table)
    id_hot = (ids[:, None] == jnp.arange(held_rows)[None, :]).astype(bf16)
    taken_hot = (picks[:, 0:1] == jnp.arange(vocab)[None, :]).astype(bf16)
    start = (dot(id_hot, replay) + dot(taken_hot, action_table)).astype(bf16)
    start_wide = start.astype(f32)
    squares = jnp.sum(start_wide * start_wide, -1, keepdims=True)

    state_cuts, ups, downs, gains = call(
        0,
        functools.partial(stage_kernel, dims),
        (to_cuts(start), to_cuts(w_down[0]), w_up[0], my_cut(norm_gain)),
        (
            ((outer, rows, cut), bf16),
            ((sections, inner, up_held, ff), bf16),
            ((sections, outer, inner, ff_held, cut), bf16),
            ((sections, 1, cut), f32),
        ),
        (),
        ((5, 2, top), (2, inner, 2, top), (4,)),
    )
    ups = ups.reshape(sections, cut, ff)
    downs = downs.reshape(sections, ff, cut)

    state = state_cuts.reshape(group_rows, cut)
    kept = []
    for layer in range(sections):
        wide = state.astype(f32)
        part = dot((wide * gains[layer]).astype(bf16), ups[layer]).astype(bf16)
        first = layer == 0
        stat = squares if first else jnp.sum(wide * wide, -1).reshape(outer, 1, rows)
        upper, actives, recips, recip = call(
            1 + layer,
            functools.partial(forward_kernel, dims, width, first),
            (part.reshape(outer, rows, ff), stat),
            (
                ((rows, ff), f32),
                ((outer, rows, ff), bf16),
                ((outer, 1, rows), f32),
                ((rows, 1), f32),
            ),
            (
                ((outer, rows, ff), bf16),
                ((outer, 1, rows), f32),
                ((1, rows), f32),
                ((rows, ff), bf16),
            ),
            ((4, 2, top), (4,)),
        )
        actives = actives.reshape(group_rows, ff)
        kept.append((state, recip, upper, actives, recips.reshape(group_rows, 1)))
        state = (wide + dot(actives, downs[layer])).astype(bf16)

    score_part = contract_last(state, table_cut).reshape(outer, rows, vocab)
    d_all, loss_row = call(
        1 + sections,
        functools.partial(head_kernel, dims, scale),
        (score_part, picks, marks[:, None]),
        (((outer, rows, vocab), bf16), ((1, 128), f32)),
        (((outer, rows, vocab), f32), ((rows, vocab), bf16)),
        ((2, 2, top), (2,)),
    )
    grad = dot(d_all.reshape(group_rows, vocab), table_cut).astype(bf16)

    grads_up, grads_down, grads_gain = [], [], []
    for layer in reversed(range(sections)):
        state, recip, upper, actives, recips = kept[layer]
        part = contract_last(grad, downs[layer]).astype(bf16).reshape(outer, rows, ff)
        d_uppers, pulls = call(
            2 + sections + layer,
            functools.partial(backward_kernel, dims, width),
            (part, upper, recip),
            (((outer, rows, ff), bf16), ((outer, 1, rows), f32)),
            (((outer, rows, ff), bf16), ((1, rows), f32), ((rows, ff), bf16)),
            ((3, 2, top), (3,)),
        )
        d_uppers = d_uppers.reshape(group_rows, ff)
        pulls = pulls.reshape(group_rows, 1)
        wide = state.astype(f32)
        ready = wide * recips
        d_normed = contract_last(d_uppers, ups[layer])
        grads_gain.append(jnp.sum(d_normed * ready, 0))
        normed = (ready * gains[layer]).astype(bf16)
        grads_up.append(contract_first(normed, d_uppers).astype(bf16))
        grads_down.append(contract_first(actives, grad).astype(bf16))
        if layer:
            grad = (
                grad.astype(f32) + d_normed * gains[layer] * recips - wide * pulls
            ).astype(bf16)

    gain_rows = jnp.stack(grads_gain[::-1])[:, None, :]
    loss_rows = jnp.broadcast_to(loss_row, (sections, 1, 128))
    small = jnp.concatenate([gain_rows, loss_rows], -1)
    others = sections - 1
    grad_up, down_got, small_got = call(
        2 + 2 * sections,
        functools.partial(finish_kernel, dims),
        (
            jnp.stack(grads_up[::-1]).reshape(sections, inner, up_held, ff),
            jnp.stack(grads_down[::-1]).reshape(sections, outer, inner, ff_held, cut),
            small,
        ),
        (
            ((up_held, ff), f32),
            ((outer, ff_held, cut), bf16),
            ((outer, 1, small_width), f32),
        ),
        (
            ((others, inner, up_held, ff), bf16),
            ((others, outer, inner, ff_held, cut), bf16),
            ((others, 1, small_width), f32),
            ((inner, up_held, ff), bf16),
            ((outer, inner, ff_held, cut), bf16),
            ((1, small_width), f32),
            ((inner - 1, up_held, ff), bf16),
            ((inner - 1, outer, ff_held, cut), bf16),
            ((inner - 1, 1, small_width), f32),
            ((outer, ff_held, cut), bf16),
            ((1, small_width), f32),
        ),
        ((8, 2, top), (2,)),
    )
    grad_down = down_got.transpose(1, 0, 2).reshape(ff_held, width).astype(f32)
    grad_gain = small_got[:, 0, :cut].reshape(1, width)
    loss = jnp.sum(small_got[:, 0, cut])
    return (grad_up[None], grad_down[None], grad_gain, loss)


def solution(mesh):
    return jax.shard_map(
        on_device,
        mesh=mesh,
        in_specs=(
            P("dp", None),
            P("dp"),
            P("dp", None),
            P("dp"),
            P(),
            P("section", None),
            P("section", "dp", None),
            P("section", "dp", None),
        ),
        out_specs=(P("section", "dp", None), P("section", "dp", None), P("section", None), P()),
        check_vma=False,
    )
```
